32 devices in a mesh: row: 8 (over y, x, core), col: 4 (over z).
Axes of the slice: x: 2, y: 2, z: 4, core: 2. Of those that a mesh axis runs over, the one named last changes fastest.
Arguments:
- points: float32 [64, 8192], P(None, ('row', 'col')), may hold values from -6 to 6
- labels: int32 [64], P(('row', 'col')), may hold values from 0 to 1
- solution: float32 [8192], P(('row', 'col')), may hold values from -6 to 6
- residual: float32 [8192], P(('row', 'col')), may hold values from -6 to 6
- direction: float32 [8192], P(('row', 'col')), may hold values from -6 to 6
- len_low: float32 [64], replicated, may hold values from 0.75 to 40
- len_high: float32 [64], replicated, may hold values from 0.9 to 40
- variances: float32 [2], replicated, may hold values from 0.5 to 2
- nugget: float32 [2], replicated, may hold values from 0.3 to 1.5
- coupling: float32 [1], replicated, may hold values from 0.6 to 1.6
Outputs:
- solution_next: float32 [8192], P(('row', 'col'))
- residual_next: float32 [8192], P(('row', 'col'))
- direction_next: float32 [8192], P(('row', 'col'))
The draws below stay inside these ranges and needn't reach their ends.
All inputs are finite; a program needn't handle non-finite values.
Results may differ from the reference program's by a relative error of at most 0.00027.
Values sent between devices are 32-bit elements; how exact they have to be, the bound alone decides.
A program may use at most 64 MiB of HBM per device.

```python
import math
import jax
import jax.numpy as jnp
from jax import lax

FEATURES = 64
NPTS = 8192
BLOCKS = 64


def draw_lengths(key, salt, short_lo, short_hi, long_lo, long_hi):
    ranking = jax.random.permutation(jax.random.fold_in(key, salt + 1), FEATURES)
    relevant = ranking < 6
    first_draw = jax.random.uniform(jax.random.fold_in(key, salt + 2), (FEATURES,), jnp.float32)
    second_draw = jax.random.uniform(jax.random.fold_in(key, salt + 3), (FEATURES,), jnp.float32)
    short_scale = jnp.exp(jnp.log(short_lo) + first_draw * (jnp.log(short_hi) - jnp.log(short_lo)))
    long_scale = jnp.exp(jnp.log(long_lo) + second_draw * (jnp.log(long_hi) - jnp.log(long_lo)))
    return jnp.where(relevant, short_scale, long_scale).astype(jnp.float32)


def draw_len_low(key, part):
    return draw_lengths(key, 100, 0.75, 1.4, 15.0, 40.0)


def draw_len_high(key, part):
    return draw_lengths(key, 200, 0.9, 1.7, 15.0, 40.0)


def draw_points(key, part):
    normals = jax.random.normal(jax.random.fold_in(key, 31), (FEATURES, NPTS), jnp.float32)
    return jnp.clip(normals, -6.0, 6.0).astype(jnp.float32)


def place_ends(drawn, key, low, high):
    place = [jax.random.randint(jax.random.fold_in(key, axis), (), 0, length) for axis, length in enumerate(drawn.shape)]
    widest = drawn.shape.index(max(drawn.shape))
    next_to = place[:widest] + [(place[widest] + 1) % drawn.shape[widest]] + place[widest + 1:]
    return drawn.at[tuple(place)].set(low).at[tuple(next_to)].set(high)


def block_levels(key, extent, split, low, high):
    level, own = 1.0, jax.random.fold_in(key, 6)
    for axis_at, shards_of in split:
        heights = jnp.exp(jax.random.uniform(jax.random.fold_in(own, axis_at), (shards_of,), jnp.float32, low / len(split), high / len(split)))
        level = level * jnp.repeat(heights, extent[axis_at] // shards_of).reshape([-1 if axis == axis_at else 1 for axis in range(len(extent))])
    return level


def noise(key, extent, deviation, reach, split=(), kind=jnp.bfloat16):
    entries = jax.random.normal(key, extent, jnp.float32) * deviation
    if len(split) > 0:
        entries = block_levels(key, extent, split, -0.22, 0.18) * entries
    return jnp.clip(entries, min=-reach, max=reach).astype(kind)


def setup_inputs(seed: int = 0) -> dict:
    splits = jax.random.split(jax.random.key(seed), 11)
    return {
        "points": draw_points(jax.random.fold_in(splits[10], 71), 0),
        "labels": place_ends(jax.random.randint(splits[1], (BLOCKS,), 0, 2), jax.random.fold_in(splits[1], 1), 0, 1).astype(jnp.int32),
        "solution": noise(splits[2], (NPTS,), 1.0, 6.0, ((0, 32),), jnp.float32),
        "residual": noise(splits[3], (NPTS,), 1.0, 6.0, ((0, 32),), jnp.float32),
        "direction": noise(splits[4], (NPTS,), 1.0, 6.0, ((0, 32),), jnp.float32),
        "len_low": draw_len_low(jax.random.fold_in(splits[10], 71), 0),
        "len_high": draw_len_high(jax.random.fold_in(splits[10], 71), 0),
        "variances": jnp.clip(jnp.exp(jax.random.uniform(splits[7], (2,), jnp.float32, math.log(0.5), math.log(2.0))), 0.5, 2.0),
        "nugget": jnp.clip(jnp.exp(jax.random.uniform(splits[8], (2,), jnp.float32, math.log(0.3), math.log(1.5))), 0.3, 1.5),
        "coupling": jnp.clip(jax.random.uniform(splits[9], (1,), jnp.float32, 0.6, 1.6), 0.6, 1.6),
    }


def point_factors(labels, coupling, nugget):
    fidelity = jnp.repeat(labels, 128).astype(jnp.float32)
    row_scale = 1.0 + (coupling[0] - 1.0) * fidelity
    nugget_points = nugget[0] + (nugget[1] - nugget[0]) * fidelity
    return row_scale, fidelity, nugget_points


def reference(points, labels, solution, residual, direction, len_low, len_high, variances, nugget, coupling):
    row_scale, high_mask, nugget_points = point_factors(labels, coupling, nugget)
    low_coords = points / len_low[:, None]
    high_coords = points / len_high[:, None]
    low_norms = jnp.sum(low_coords * low_coords, 0)
    high_norms = jnp.sum(high_coords * high_coords, 0)
    weights_low = row_scale * direction
    weights_high = high_mask * direction
    point_count = points.shape[1]
    row_block = 1024
    numbers = (point_count // row_block)
    dims = (((0,), (0,)), ((), ()))

    def block_rows(block_index):
        offset = block_index * row_block
        block_low = lax.dynamic_slice_in_dim(low_coords, offset, row_block, 1)
        block_high = lax.dynamic_slice_in_dim(high_coords, offset, row_block, 1)
        norm_low = lax.dynamic_slice_in_dim(low_norms, offset, row_block, 0)
        norm_high = lax.dynamic_slice_in_dim(high_norms, offset, row_block, 0)
        dist_low = norm_low[:, None] + low_norms[None, :] - 2.0 * lax.dot_general(
            block_low, low_coords, dims, precision=lax.Precision.HIGHEST)
        dist_high = norm_high[:, None] + high_norms[None, :] - 2.0 * lax.dot_general(
            block_high, high_coords, dims, precision=lax.Precision.HIGHEST)
        sum_low = jnp.dot(jnp.exp(-0.5 * dist_low), weights_low, precision=lax.Precision.HIGHEST)
        sum_high = jnp.dot(jnp.exp(-0.5 * dist_high), weights_high, precision=lax.Precision.HIGHEST)
        return sum_low, sum_high

    sum_low, sum_high = lax.map(block_rows, jnp.arange(numbers, dtype=jnp.int32))
    sum_low = sum_low.reshape(-1)
    sum_high = sum_high.reshape(-1)
    kernel_image = variances[0] * row_scale * sum_low + variances[1] * high_mask * sum_high + nugget_points * direction
    old_norm = jnp.sum(residual * residual)
    curvature = jnp.sum(direction * kernel_image)
    step_size = old_norm / curvature
    solution_next = solution + step_size * direction
    residual_next = residual - step_size * kernel_image
    new_norm = jnp.sum(residual_next * residual_next)
    direction_next = residual_next + (new_norm / old_norm) * direction
    return solution_next, residual_next, direction_next
```

```python
import functools
import math

import jax
import jax.numpy as jnp
from jax import lax
from jax.experimental import pallas as pl
from jax.experimental.pallas import tpu as pltpu
from jax.sharding import PartitionSpec as P

MESH = pl.DeviceIdType.MESH
LANES = 128
ROOT_LOG2E = math.sqrt(math.log2(math.e))


def peer_of(index, offset, count):
    if count & (count - 1):
        return lax.rem(index + offset, count)
    peer, bit = index, 1
    while bit < count:
        if offset & bit:
            peer = peer + bit * (1 - 2 * ((index // bit) % 2))
        bit *= 2
    return peer


def as_column(row):
    n = row.shape[1]
    diagonal = lax.broadcasted_iota(jnp.int32, (n, n), 0) == lax.broadcasted_iota(
        jnp.int32, (n, n), 1
    )
    return jnp.sum(jnp.where(diagonal, jnp.broadcast_to(row, (n, n)), 0.0), axis=1, keepdims=True)


def two_terms(value):
    hi = value.astype(jnp.bfloat16)
    lo = (value - hi.astype(jnp.float32)).astype(jnp.bfloat16)
    whole = hi.astype(jnp.float32) + lo.astype(jnp.float32)
    return hi, lo, whole


def kernel(
    row_count,
    col_count,
    points_ref,
    labels_ref,
    solution_ref,
    residual_ref,
    direction_ref,
    len_low_ref,
    len_high_ref,
    variances_ref,
    nugget_ref,
    coupling_ref,
    solution_out,
    residual_out,
    direction_out,
    col_buf,
    row_buf,
    lhs,
    rhs,
    col_bias,
    col_weight,
    part_buf,
    sums_buf,
    row_send,
    row_recv,
    col_send,
    col_recv,
    part_send,
    part_recv,
    sums_send,
    sums_recv,
):
    me_row, me_col = lax.axis_index("row"), lax.axis_index("col")
    features, width = points_ref.shape
    row_peers = [(d, (peer_of(me_row, d, row_count), me_col)) for d in range(1, row_count)]
    col_peers = [(d, (me_row, peer_of(me_col, d, col_count))) for d in range(1, col_count)]

    barrier = pltpu.get_barrier_semaphore()
    for _, peer in row_peers + col_peers:
        pl.semaphore_signal(barrier, inc=1, device_id=peer, device_id_type=MESH)

    own = col_buf.at[0]
    lane = lax.broadcasted_iota(jnp.int32, (1, width), 1)
    fidelity = jnp.zeros((1, width), jnp.float32)
    for block in range(labels_ref.shape[0]):
        fidelity = jnp.where(
            lane // LANES == block, labels_ref[block].astype(jnp.float32), fidelity
        )
    own[:features, :] = points_ref[...]
    own[features:, :] = jnp.concatenate(
        [fidelity, direction_ref[...], residual_ref[...], jnp.zeros((5, width), jnp.float32)], 0
    )
    row_buf[0] = own[...]

    pl.semaphore_wait(barrier, len(row_peers) + len(col_peers))

    sends = []
    for d, peer in col_peers:
        sends.append(
            pltpu.make_async_remote_copy(
                src_ref=own,
                dst_ref=row_buf.at[d],
                send_sem=col_send.at[d],
                recv_sem=col_recv.at[d],
                device_id=peer,
                device_id_type=MESH,
            )
        )
        sends[-1].start()
    col_copies = dict(zip([d for d, _ in col_peers], sends))
    row_copies = {}
    for d, peer in row_peers:
        copy = pltpu.make_async_remote_copy(
            src_ref=own,
            dst_ref=col_buf.at[d],
            send_sem=row_send.at[d],
            recv_sem=row_recv.at[d],
            device_id=peer,
            device_id_type=MESH,
        )
        copy.start()
        row_copies[d] = copy

    inverse = [ROOT_LOG2E / len_low_ref[...], ROOT_LOG2E / len_high_ref[...]]
    lane_scale = [jnp.concatenate([value, value], 1) for value in inverse]
    column_scale = [as_column(value) for value in inverse]
    coupling = coupling_ref[0]

    def prepare_rows(d):
        raw = row_buf[d, :features, :]
        for which in range(2):
            hi, lo, whole = two_terms(raw * column_scale[which])
            rhs[which] = jnp.concatenate([hi, lo, hi, lo], 0)
            yield -0.5 * jnp.sum(whole * whole, 0, keepdims=True)

    def prepare_columns(d):
        raw = col_buf[d, :features, :]
        turned = jnp.concatenate([raw, raw], 0).T
        extra = jnp.concatenate(
            [col_buf[d, features:, :], jnp.zeros((LANES - 8, width), jnp.float32)], 0
        ).T
        label, step_dir = extra[:, 0:1], extra[:, 1:2]
        weights = [(1.0 + (coupling - 1.0) * label) * step_dir, label * step_dir]
        for which in range(2):
            hi, lo, whole = two_terms(turned * lane_scale[which])
            lhs[which, d] = jnp.concatenate([hi, lo], 1)
            bias = -0.25 * jnp.sum(whole * whole, 1, keepdims=True)
            col_bias[which, d] = jnp.broadcast_to(bias, (width, LANES))
            col_weight[which, d] = jnp.broadcast_to(weights[which], (width, LANES))

    def accumulate(d, row_bias, totals):
        result = []
        for which in range(2):
            power = jnp.dot(lhs[which, d], rhs[which], preferred_element_type=jnp.float32)
            bias, weight = col_bias[which, d], col_weight[which, d]
            halves = []
            for at in range(0, width, LANES):
                value = (
                    jnp.exp2(power[:, at : at + LANES] + bias + row_bias[which][:, at : at + LANES])
                    * weight
                )
                halves.append(jnp.sum(value.reshape(width // 8, 8, LANES), 0))
            result.append(totals[which] + jnp.concatenate(halves, 1))
        return tuple(result)

    zeros = jnp.zeros((8, width), jnp.float32)

    def finish(d, totals):
        label = row_buf[d, features : features + 1, :]
        low = jnp.sum(totals[0], 0, keepdims=True)
        high = jnp.sum(totals[1], 0, keepdims=True)
        part_buf[0, d : d + 1, :] = (
            variances_ref[0] * (1.0 + (coupling - 1.0) * label) * low
            + variances_ref[1] * label * high
        )

    row_bias = list(prepare_rows(0))
    totals = (zeros, zeros)
    prepare_columns(0)
    totals = accumulate(0, row_bias, totals)
    for d in range(1, row_count):
        row_copies[d].wait_recv()
        prepare_columns(d)
        totals = accumulate(d, row_bias, totals)
    finish(0, totals)
    for c in range(1, col_count):
        col_copies[c].wait_recv()
        row_bias = list(prepare_rows(c))
        totals = lax.fori_loop(
            0, row_count, lambda d, t: accumulate(d, row_bias, t), (zeros, zeros)
        )
        finish(c, totals)

    part_copies = []
    for d, peer in col_peers:
        copy = pltpu.make_async_remote_copy(
            src_ref=part_buf.at[0],
            dst_ref=part_buf.at[d],
            send_sem=part_send.at[d],
            recv_sem=part_recv.at[d],
            device_id=peer,
            device_id_type=MESH,
        )
        copy.start()
        part_copies.append(copy)

    first, second = nugget_ref[0], nugget_ref[1]
    images, labels_of, dirs, resids = [], [], [], []
    for d in range(col_count):
        labels_of.append(row_buf[d, features : features + 1, :])
        dirs.append(row_buf[d, features + 1 : features + 2, :])
        resids.append(row_buf[d, features + 2 : features + 3, :])
        images.append(
            part_buf[0, d : d + 1, :] + (first + (second - first) * labels_of[d]) * dirs[d]
        )
    for d, copy in enumerate(part_copies, 1):
        copy.wait_recv()
        for e in range(col_count):
            if col_count & (col_count - 1):
                place = (e - d) % col_count
                images[e] = images[e] + part_buf[d, place : place + 1, :]
            else:
                images[e] = images[e] + part_buf[d, (d ^ e) : (d ^ e) + 1, :]

    def line_sum(left, right):
        total = sum(a * b for a, b in zip(left, right))
        return sum(total[:, at : at + LANES] for at in range(0, width, LANES))

    sums_buf[0] = jnp.concatenate(
        [
            line_sum(resids, resids),
            line_sum(dirs, images),
            line_sum(resids, images),
            line_sum(images, images),
            jnp.zeros((4, LANES), jnp.float32),
        ],
        0,
    )
    sums_copies = []
    for d, peer in row_peers:
        copy = pltpu.make_async_remote_copy(
            src_ref=sums_buf.at[0],
            dst_ref=sums_buf.at[d],
            send_sem=sums_send.at[d],
            recv_sem=sums_recv.at[d],
            device_id=peer,
            device_id_type=MESH,
        )
        copy.start()
        sums_copies.append(copy)
    sums = sums_buf[0]
    for d, copy in enumerate(sums_copies, 1):
        copy.wait_recv()
        sums = sums + sums_buf[d]
    sums = jnp.sum(sums, 1, keepdims=True)
    old_norm, curvature = sums[0:1], sums[1:2]
    cross_term, image_norm = sums[2:3], sums[3:4]
    step_size = old_norm / curvature
    new_norm = old_norm - 2.0 * step_size * cross_term + step_size * step_size * image_norm
    residual_next = resids[0] - step_size * images[0]
    solution_out[...] = solution_ref[...] + step_size * dirs[0]
    residual_out[...] = residual_next
    direction_out[...] = residual_next + new_norm / old_norm * dirs[0]

    for copy in sends + list(row_copies.values()) + part_copies + sums_copies:
        copy.wait_send()


def solution(mesh):
    row_count, col_count = mesh.shape["row"], mesh.shape["col"]

    def body(points, labels, solution, residual, direction, len_low, len_high, *scalars):
        features, width = points.shape
        height = features + 8
        vector = jax.ShapeDtypeStruct((1, width), jnp.float32)
        vmem = pl.BlockSpec(memory_space=pltpu.VMEM)
        smem = pl.BlockSpec(memory_space=pltpu.SMEM)
        dma = pltpu.SemaphoreType.DMA
        outs = pl.pallas_call(
            functools.partial(kernel, row_count, col_count),
            out_shape=(vector,) * 3,
            in_specs=[vmem, smem, vmem, vmem, vmem, vmem, vmem, smem, smem, smem],
            out_specs=(vmem,) * 3,
            scratch_shapes=[
                pltpu.VMEM((row_count, height, width), jnp.float32),
                pltpu.VMEM((col_count, height, width), jnp.float32),
                pltpu.VMEM((2, row_count, width, 4 * features), jnp.bfloat16),
                pltpu.VMEM((2, 4 * features, width), jnp.bfloat16),
                pltpu.VMEM((2, row_count, width, LANES), jnp.float32),
                pltpu.VMEM((2, row_count, width, LANES), jnp.float32),
                pltpu.VMEM((col_count, max(col_count, 8), width), jnp.float32),
                pltpu.VMEM((row_count, 8, LANES), jnp.float32),
                dma((row_count,)),
                dma((row_count,)),
                dma((col_count,)),
                dma((col_count,)),
                dma((col_count,)),
                dma((col_count,)),
                dma((row_count,)),
                dma((row_count,)),
            ],
            compiler_params=pltpu.CompilerParams(
                collective_id=0, has_side_effects=True, vmem_limit_bytes=48 * 1024 * 1024
            ),
        )(
            points,
            labels,
            solution.reshape(1, -1),
            residual.reshape(1, -1),
            direction.reshape(1, -1),
            len_low.reshape(1, -1),
            len_high.reshape(1, -1),
            *scalars,
        )
        return tuple(out.reshape(-1) for out in outs)

    spread = P(("row", "col"))
    return jax.shard_map(
        body,
        mesh=mesh,
        in_specs=(P(None, ("row", "col")), spread, spread, spread, spread) + (P(),) * 5,
        out_specs=(spread,) * 3,
        check_vma=False,
    )
```

```python
import functools
import math

import jax
import jax.numpy as jnp
from jax import lax
from jax.experimental import pallas as pl
from jax.experimental.pallas import tpu as pltpu
from jax.sharding import PartitionSpec as P

MESH = pl.DeviceIdType.MESH
LANES = 128
ROOT_LOG2E = math.sqrt(math.log2(math.e))


def peer_of(index, offset, count):
    if count & (count - 1):
        return lax.rem(index + offset, count)
    peer, bit = index, 1
    while bit < count:
        if offset & bit:
            peer = peer + bit * (1 - 2 * ((index // bit) % 2))
        bit *= 2
    return peer


def as_column(row):
    n = row.shape[1]
    diagonal = lax.broadcasted_iota(jnp.int32, (n, n), 0) == lax.broadcasted_iota(
        jnp.int32, (n, n), 1
    )
    return jnp.sum(jnp.where(diagonal, jnp.broadcast_to(row, (n, n)), 0.0), axis=1, keepdims=True)


def two_terms(value):
    hi = value.astype(jnp.bfloat16)
    lo = (value - hi.astype(jnp.float32)).astype(jnp.bfloat16)
    whole = hi.astype(jnp.float32) + lo.astype(jnp.float32)
    return hi, lo, whole


def kernel(
    row_count,
    col_count,
    points_hbm,
    labels_hbm,
    residual_hbm,
    direction_hbm,
    len_low_hbm,
    len_high_hbm,
    variances_hbm,
    nugget_hbm,
    coupling_hbm,
    image_out,
    step_out,
    ratio_out,
    labels_ref,
    residual_ref,
    direction_ref,
    len_low_ref,
    len_high_ref,
    variances_ref,
    nugget_ref,
    coupling_ref,
    load_sem,
    col_buf,
    row_buf,
    lhs,
    rhs,
    col_bias,
    col_weight,
    part_buf,
    sums_buf,
    row_send,
    row_recv,
    col_send,
    col_recv,
    part_send,
    part_recv,
    sums_send,
    sums_recv,
):
    me_row, me_col = lax.axis_index("row"), lax.axis_index("col")
    features, width = points_hbm.shape
    row_peers = [(d, (peer_of(me_row, d, row_count), me_col)) for d in range(1, row_count)]
    col_peers = [(d, (me_row, peer_of(me_col, d, col_count))) for d in range(1, col_count)]

    barrier = pltpu.get_barrier_semaphore()
    for _, peer in row_peers + col_peers:
        pl.semaphore_signal(barrier, inc=1, device_id=peer, device_id_type=MESH)

    own = col_buf.at[0]
    loads = [
        pltpu.make_async_copy(source, target, load_sem.at[at])
        for at, (source, target) in enumerate(
            [
                (points_hbm, own.at[:features, :]),
                (labels_hbm, labels_ref),
                (direction_hbm, direction_ref),
                (residual_hbm, residual_ref),
                (len_low_hbm, len_low_ref),
                (len_high_hbm, len_high_ref),
                (variances_hbm, variances_ref),
                (nugget_hbm, nugget_ref),
                (coupling_hbm, coupling_ref),
            ]
        )
    ]
    for load in loads:
        load.start()
    for load in loads:
        load.wait()
    lane = lax.broadcasted_iota(jnp.int32, (1, width), 1)
    labels = labels_ref[...].astype(jnp.float32)
    fidelity = jnp.zeros((1, width), jnp.float32)
    for block in range(labels.shape[1]):
        fidelity = jnp.where(lane // LANES == block, labels[:, block : block + 1], fidelity)
    own[features:, :] = jnp.concatenate(
        [fidelity, direction_ref[...], residual_ref[...], jnp.zeros((5, width), jnp.float32)], 0
    )

    pl.semaphore_wait(barrier, len(row_peers) + len(col_peers))

    sends = []
    for d, peer in col_peers:
        sends.append(
            pltpu.make_async_remote_copy(
                src_ref=own,
                dst_ref=row_buf.at[d],
                send_sem=col_send.at[d],
                recv_sem=col_recv.at[d],
                device_id=peer,
                device_id_type=MESH,
            )
        )
        sends[-1].start()
    col_copies = dict(zip([d for d, _ in col_peers], sends))
    row_copies = {}

    def send_row(source, d, slot):
        copy = pltpu.make_async_remote_copy(
            src_ref=source,
            dst_ref=col_buf.at[slot],
            send_sem=row_send.at[slot],
            recv_sem=row_recv.at[slot],
            device_id=(peer_of(me_row, d, row_count), me_col),
            device_id_type=MESH,
        )
        copy.start()
        row_copies[slot] = copy

    paired = row_count > 1 and row_count & (row_count - 1) == 0
    straight = [d for d in range(2, row_count, 2)] + [1] if paired else list(range(1, row_count))
    for d in straight:
        send_row(own, d, d)

    inverse = [ROOT_LOG2E / len_low_ref[...], ROOT_LOG2E / len_high_ref[...]]
    lane_scale = [jnp.concatenate([value, value], 1) for value in inverse]
    column_scale = [as_column(value) for value in inverse]
    coupling = coupling_ref[...]
    row_blocks = [own] + [row_buf.at[d] for d in range(1, col_count)]

    def prepare_rows(d):
        raw = row_blocks[d][:features, :]
        for which in range(2):
            hi, lo, whole = two_terms(raw * column_scale[which])
            rhs[which] = jnp.concatenate([hi, lo, hi, lo], 0)
            yield -0.5 * jnp.sum(whole * whole, 0, keepdims=True)

    def prepare_columns(d):
        raw = col_buf[d, :features, :]
        turned = jnp.concatenate([raw, raw], 0).T
        extra = jnp.concatenate(
            [col_buf[d, features:, :], jnp.zeros((LANES - 8, width), jnp.float32)], 0
        ).T
        label, step_dir = extra[:, 0:1], extra[:, 1:2]
        weights = [(1.0 + (coupling - 1.0) * label) * step_dir, label * step_dir]
        for which in range(2):
            hi, lo, whole = two_terms(turned * lane_scale[which])
            lhs[which, d] = jnp.concatenate([hi, lo], 1)
            bias = -0.25 * jnp.sum(whole * whole, 1, keepdims=True)
            col_bias[which, d] = jnp.broadcast_to(bias, (width, LANES))
            col_weight[which, d] = jnp.broadcast_to(weights[which], (width, LANES))

    def accumulate(d, row_bias, totals):
        result = []
        for which in range(2):
            power = jnp.dot(lhs[which, d], rhs[which], preferred_element_type=jnp.float32)
            bias, weight = col_bias[which, d], col_weight[which, d]
            halves = []
            for at in range(0, width, LANES):
                value = (
                    jnp.exp2(power[:, at : at + LANES] + bias + row_bias[which][:, at : at + LANES])
                    * weight
                )
                halves.append(jnp.sum(value.reshape(width // 8, 8, LANES), 0))
            result.append(totals[which] + jnp.concatenate(halves, 1))
        return tuple(result)

    zeros = jnp.zeros((8, width), jnp.float32)

    def finish(d, totals):
        label = row_blocks[d][features : features + 1, :]
        low = jnp.sum(totals[0], 0, keepdims=True)
        high = jnp.sum(totals[1], 0, keepdims=True)
        part_buf[0, d : d + 1, :] = (
            variances_ref[:, 0:1] * (1.0 + (coupling - 1.0) * label) * low
            + variances_ref[:, 1:2] * label * high
        )

    row_bias = list(prepare_rows(0))
    totals = (zeros, zeros)
    prepare_columns(0)
    totals = accumulate(0, row_bias, totals)
    if paired:
        order = [1] + straight[:-1]
        for d in order:
            row_copies[d].wait_recv()
            if d > 1:
                send_row(col_buf.at[d], 1, d + 1)
            prepare_columns(d)
            totals = accumulate(d, row_bias, totals)
        rest = list(range(3, row_count, 2))
    else:
        rest = list(range(1, row_count))
    for d in rest:
        row_copies[d].wait_recv()
        prepare_columns(d)
        totals = accumulate(d, row_bias, totals)
    finish(0, totals)
    for c in range(1, col_count):
        col_copies[c].wait_recv()
        row_bias = list(prepare_rows(c))
        totals = lax.fori_loop(
            0, row_count, lambda d, t: accumulate(d, row_bias, t), (zeros, zeros), unroll=True
        )
        finish(c, totals)

    part_copies = []
    for d, peer in col_peers:
        copy = pltpu.make_async_remote_copy(
            src_ref=part_buf.at[0],
            dst_ref=part_buf.at[d],
            send_sem=part_send.at[d],
            recv_sem=part_recv.at[d],
            device_id=peer,
            device_id_type=MESH,
        )
        copy.start()
        part_copies.append(copy)

    first, second = nugget_ref[:, 0:1], nugget_ref[:, 1:2]
    images, labels_of, dirs, resids = [], [], [], []
    for d in range(col_count):
        labels_of.append(row_blocks[d][features : features + 1, :])
        dirs.append(row_blocks[d][features + 1 : features + 2, :])
        resids.append(row_blocks[d][features + 2 : features + 3, :])
        images.append(
            part_buf[0, d : d + 1, :] + (first + (second - first) * labels_of[d]) * dirs[d]
        )
    for d, copy in enumerate(part_copies, 1):
        copy.wait_recv()
        for e in range(col_count):
            if col_count & (col_count - 1):
                place = (e - d) % col_count
                images[e] = images[e] + part_buf[d, place : place + 1, :]
            else:
                images[e] = images[e] + part_buf[d, (d ^ e) : (d ^ e) + 1, :]

    def line_sum(left, right):
        total = sum(a * b for a, b in zip(left, right))
        return sum(total[:, at : at + LANES] for at in range(0, width, LANES))

    sums_buf[0] = jnp.concatenate(
        [
            line_sum(resids, resids),
            line_sum(dirs, images),
            line_sum(resids, images),
            line_sum(images, images),
            jnp.zeros((4, LANES), jnp.float32),
        ],
        0,
    )
    sums_copies = []
    for d, peer in row_peers:
        copy = pltpu.make_async_remote_copy(
            src_ref=sums_buf.at[0],
            dst_ref=sums_buf.at[d],
            send_sem=sums_send.at[d],
            recv_sem=sums_recv.at[d],
            device_id=peer,
            device_id_type=MESH,
        )
        copy.start()
        sums_copies.append(copy)
    sums = sums_buf[0]
    for d, copy in enumerate(sums_copies, 1):
        copy.wait_recv()
        sums = sums + sums_buf[d]
    sums = jnp.sum(sums, 1, keepdims=True)
    old_norm, curvature = sums[0:1], sums[1:2]
    cross_term, image_norm = sums[2:3], sums[3:4]
    step_size = old_norm / curvature
    new_norm = old_norm - 2.0 * step_size * cross_term + step_size * step_size * image_norm
    image_out[...] = images[0]
    step_out[...] = jnp.broadcast_to(step_size, (1, width))
    ratio_out[...] = jnp.broadcast_to(new_norm / old_norm, (1, width))

    for copy in sends + list(row_copies.values()) + part_copies + sums_copies:
        copy.wait_send()


def solution(mesh):
    row_count, col_count = mesh.shape["row"], mesh.shape["col"]

    def body(points, labels, solution, residual, direction, len_low, len_high, *scalars):
        features, width = points.shape
        height = features + 8
        vmem = pl.BlockSpec(memory_space=pltpu.VMEM)
        dma = pltpu.SemaphoreType.DMA
        operands = [points] + [
            value.reshape(1, -1)
            for value in (labels, residual, direction, len_low, len_high, *scalars)
        ]
        image, step_size, ratio = pl.pallas_call(
            functools.partial(kernel, row_count, col_count),
            out_shape=(jax.ShapeDtypeStruct((1, width), jnp.float32),) * 3,
            in_specs=[pl.BlockSpec(memory_space=pltpu.HBM)] * len(operands),
            out_specs=(vmem,) * 3,
            scratch_shapes=[pltpu.VMEM(value.shape, value.dtype) for value in operands[1:]]
            + [
                dma((len(operands),)),
                pltpu.VMEM((row_count, height, width), jnp.float32),
                pltpu.VMEM((col_count, height, width), jnp.float32),
                pltpu.VMEM((2, row_count, width, 4 * features), jnp.bfloat16),
                pltpu.VMEM((2, 4 * features, width), jnp.bfloat16),
                pltpu.VMEM((2, row_count, width, LANES), jnp.float32),
                pltpu.VMEM((2, row_count, width, LANES), jnp.float32),
                pltpu.VMEM((col_count, max(col_count, 8), width), jnp.float32),
                pltpu.VMEM((row_count, 8, LANES), jnp.float32),
                dma((row_count,)),
                dma((row_count,)),
                dma((col_count,)),
                dma((col_count,)),
                dma((col_count,)),
                dma((col_count,)),
                dma((row_count,)),
                dma((row_count,)),
            ],
            compiler_params=pltpu.CompilerParams(
                collective_id=0, has_side_effects=True
            ),
        )(*operands)
        image, step_size, ratio = (value.reshape(-1) for value in (image, step_size, ratio))
        residual_next = residual - step_size * image
        return solution + step_size * direction, residual_next, residual_next + ratio * direction

    spread = P(("row", "col"))
    return jax.shard_map(
        body,
        mesh=mesh,
        in_specs=(P(None, ("row", "col")), spread, spread, spread, spread) + (P(),) * 5,
        out_specs=(spread,) * 3,
        check_vma=False,
    )
```

```python
import functools
import math

import jax
import jax.numpy as jnp
from jax import lax
from jax.experimental import pallas as pl
from jax.experimental.pallas import tpu as pltpu
from jax.sharding import PartitionSpec as P

MESH = pl.DeviceIdType.MESH
LANES = 128
ROOT_LOG2E = math.sqrt(math.log2(math.e))


def peer_of(index, offset, count):
    if count & (count - 1):
        return lax.rem(index + offset, count)
    peer, bit = index, 1
    while bit < count:
        if offset & bit:
            peer = peer + bit * (1 - 2 * ((index // bit) % 2))
        bit *= 2
    return peer


def as_column(row):
    n = row.shape[1]
    diagonal = lax.broadcasted_iota(jnp.int32, (n, n), 0) == lax.broadcasted_iota(
        jnp.int32, (n, n), 1
    )
    return jnp.sum(jnp.where(diagonal, jnp.broadcast_to(row, (n, n)), 0.0), axis=1, keepdims=True)


def two_terms(value):
    hi = value.astype(jnp.bfloat16)
    lo = (value - hi.astype(jnp.float32)).astype(jnp.bfloat16)
    whole = hi.astype(jnp.float32) + lo.astype(jnp.float32)
    return hi, lo, whole


def kernel(
    row_count,
    col_count,
    points_hbm,
    labels_hbm,
    residual_hbm,
    direction_hbm,
    len_low_hbm,
    len_high_hbm,
    variances_hbm,
    nugget_hbm,
    coupling_hbm,
    image_out,
    step_out,
    ratio_out,
    labels_ref,
    residual_ref,
    direction_ref,
    len_low_ref,
    len_high_ref,
    variances_ref,
    nugget_ref,
    coupling_ref,
    load_sem,
    col_buf,
    row_buf,
    lhs,
    rhs,
    col_bias,
    col_weight,
    part_buf,
    sums_buf,
    row_send,
    row_recv,
    col_send,
    col_recv,
    part_send,
    part_recv,
    sums_send,
    sums_recv,
):
    me_row, me_col = lax.axis_index("row"), lax.axis_index("col")
    features, width = points_hbm.shape
    row_peers = [(d, (peer_of(me_row, d, row_count), me_col)) for d in range(1, row_count)]
    col_peers = [(d, (me_row, peer_of(me_col, d, col_count))) for d in range(1, col_count)]

    barrier = pltpu.get_barrier_semaphore()
    for _, peer in row_peers + col_peers:
        pl.semaphore_signal(barrier, inc=1, device_id=peer, device_id_type=MESH)

    own = col_buf.at[0]
    loads = [
        pltpu.make_async_copy(source, target, load_sem.at[at])
        for at, (source, target) in enumerate(
            [
                (points_hbm, own.at[:features, :]),
                (labels_hbm, labels_ref),
                (direction_hbm, direction_ref),
                (residual_hbm, residual_ref),
                (len_low_hbm, len_low_ref),
                (len_high_hbm, len_high_ref),
                (variances_hbm, variances_ref),
                (nugget_hbm, nugget_ref),
                (coupling_hbm, coupling_ref),
            ]
        )
    ]
    for load in loads:
        load.start()
    for load in loads:
        load.wait()
    lane = lax.broadcasted_iota(jnp.int32, (1, width), 1)
    labels = labels_ref[...].astype(jnp.float32)
    fidelity = jnp.zeros((1, width), jnp.float32)
    for block in range(labels.shape[1]):
        fidelity = jnp.where(lane // LANES == block, labels[:, block : block + 1], fidelity)
    own[features:, :] = jnp.concatenate(
        [fidelity, direction_ref[...], residual_ref[...], jnp.zeros((5, width), jnp.float32)], 0
    )

    pl.semaphore_wait(barrier, len(row_peers) + len(col_peers))

    col_order = [0] + [col_count - 1][: col_count - 1] + list(range(1, col_count - 1))
    sends = []
    for d, peer in [col_peers[d - 1] for d in col_order[1:]]:
        sends.append(
            pltpu.make_async_remote_copy(
                src_ref=own,
                dst_ref=row_buf.at[d],
                send_sem=col_send.at[d],
                recv_sem=col_recv.at[d],
                device_id=peer,
                device_id_type=MESH,
            )
        )
        sends[-1].start()
    col_copies = dict(zip(col_order[1:], sends))
    row_copies = {}

    def send_row(source, d, slot):
        copy = pltpu.make_async_remote_copy(
            src_ref=source,
            dst_ref=col_buf.at[slot],
            send_sem=row_send.at[slot],
            recv_sem=row_recv.at[slot],
            device_id=(peer_of(me_row, d, row_count), me_col),
            device_id_type=MESH,
        )
        copy.start()
        row_copies[slot] = copy

    paired = row_count > 1 and row_count & (row_count - 1) == 0
    straight = [d for d in range(2, row_count, 2)] + [1] if paired else list(range(1, row_count))
    for d in straight:
        send_row(own, d, d)

    inverse = [ROOT_LOG2E / len_low_ref[...], ROOT_LOG2E / len_high_ref[...]]
    lane_scale = [jnp.concatenate([value, value], 1) for value in inverse]
    column_scale = [as_column(value) for value in inverse]
    coupling = coupling_ref[...]
    row_blocks = [own] + [row_buf.at[d] for d in range(1, col_count)]

    def prepare_rows(d):
        raw = row_blocks[d][:features, :]
        for which in range(2):
            hi, lo, whole = two_terms(raw * column_scale[which])
            rhs[which] = jnp.concatenate([hi, lo, hi, lo], 0)
            yield -0.5 * jnp.sum(whole * whole, 0, keepdims=True)

    def prepare_columns(d):
        raw = col_buf[d, :features, :]
        turned = jnp.concatenate([raw, raw], 0).T
        extra = jnp.concatenate(
            [col_buf[d, features:, :], jnp.zeros((LANES - 8, width), jnp.float32)], 0
        ).T
        label, step_dir = extra[:, 0:1], extra[:, 1:2]
        weights = [(1.0 + (coupling - 1.0) * label) * step_dir, label * step_dir]
        for which in range(2):
            hi, lo, whole = two_terms(turned * lane_scale[which])
            lhs[which, d] = jnp.concatenate([hi, lo], 1)
            bias = -0.25 * jnp.sum(whole * whole, 1, keepdims=True)
            col_bias[which, d] = jnp.broadcast_to(bias, (width, LANES))
            col_weight[which, d] = jnp.broadcast_to(weights[which], (width, LANES))

    def accumulate(d, row_bias, totals):
        result = []
        for which in range(2):
            power = jnp.dot(lhs[which, d], rhs[which], preferred_element_type=jnp.float32)
            bias, weight = col_bias[which, d], col_weight[which, d]
            halves = []
            for at in range(0, width, LANES):
                value = (
                    jnp.exp2(power[:, at : at + LANES] + bias + row_bias[which][:, at : at + LANES])
                    * weight
                )
                halves.append(jnp.sum(value.reshape(width // 8, 8, LANES), 0))
            result.append(totals[which] + jnp.concatenate(halves, 1))
        return tuple(result)

    zeros = jnp.zeros((8, width), jnp.float32)
    part_copies = {}

    def finish(d, totals):
        label = row_blocks[d][features : features + 1, :]
        low = jnp.sum(totals[0], 0, keepdims=True)
        high = jnp.sum(totals[1], 0, keepdims=True)
        part_buf[0, d] = (
            variances_ref[:, 0:1] * (1.0 + (coupling - 1.0) * label) * low
            + variances_ref[:, 1:2] * label * high
        )
        for e, peer in col_peers:
            copy = pltpu.make_async_remote_copy(
                src_ref=part_buf.at[0, d],
                dst_ref=part_buf.at[e, d],
                send_sem=part_send.at[e, d],
                recv_sem=part_recv.at[e, d],
                device_id=peer,
                device_id_type=MESH,
            )
            copy.start()
            part_copies[e, d] = copy

    row_bias = list(prepare_rows(0))
    totals = (zeros, zeros)
    prepare_columns(0)
    totals = accumulate(0, row_bias, totals)
    if paired:
        order = [1] + straight[:-1]
        for d in order:
            row_copies[d].wait_recv()
            if d > 1:
                send_row(col_buf.at[d], 1, d + 1)
            prepare_columns(d)
            totals = accumulate(d, row_bias, totals)
        rest = list(range(3, row_count, 2))
    else:
        rest = list(range(1, row_count))
    for d in rest:
        row_copies[d].wait_recv()
        prepare_columns(d)
        totals = accumulate(d, row_bias, totals)
    finish(0, totals)
    for c in col_order[1:]:
        col_copies[c].wait_recv()
        row_bias = list(prepare_rows(c))
        totals = lax.fori_loop(
            0, row_count, lambda d, t: accumulate(d, row_bias, t), (zeros, zeros), unroll=True
        )
        finish(c, totals)

    first, second = nugget_ref[:, 0:1], nugget_ref[:, 1:2]
    images, labels_of, dirs, resids = [], [], [], []
    for d in range(col_count):
        labels_of.append(row_blocks[d][features : features + 1, :])
        dirs.append(row_blocks[d][features + 1 : features + 2, :])
        resids.append(row_blocks[d][features + 2 : features + 3, :])
        images.append(
            part_buf[0, d] + (first + (second - first) * labels_of[d]) * dirs[d]
        )
    for place in col_order:
        for d in range(1, col_count):
            e = place ^ d if col_count & (col_count - 1) == 0 else (place + d) % col_count
            part_copies[d, place].wait_recv()
            images[e] = images[e] + part_buf[d, place]

    def line_sum(left, right):
        total = sum(a * b for a, b in zip(left, right))
        return sum(total[:, at : at + LANES] for at in range(0, width, LANES))

    sums_buf[0] = jnp.concatenate(
        [
            line_sum(resids, resids),
            line_sum(dirs, images),
            line_sum(resids, images),
            line_sum(images, images),
        ],
        0,
    )
    sums_copies = []
    for d, peer in row_peers:
        copy = pltpu.make_async_remote_copy(
            src_ref=sums_buf.at[0],
            dst_ref=sums_buf.at[d],
            send_sem=sums_send.at[d],
            recv_sem=sums_recv.at[d],
            device_id=peer,
            device_id_type=MESH,
        )
        copy.start()
        sums_copies.append(copy)
    sums = sums_buf[0]
    for d, copy in enumerate(sums_copies, 1):
        copy.wait_recv()
        sums = sums + sums_buf[d]
    sums = jnp.sum(sums, 1, keepdims=True)
    old_norm, curvature = sums[0:1], sums[1:2]
    cross_term, image_norm = sums[2:3], sums[3:4]
    step_size = old_norm / curvature
    new_norm = old_norm - 2.0 * step_size * cross_term + step_size * step_size * image_norm
    image_out[...] = images[0]
    step_out[...] = jnp.broadcast_to(step_size, (1, width))
    ratio_out[...] = jnp.broadcast_to(new_norm / old_norm, (1, width))

    for copy in sends + [*row_copies.values(), *part_copies.values()] + sums_copies:
        copy.wait_send()


def solution(mesh):
    row_count, col_count = mesh.shape["row"], mesh.shape["col"]

    def body(points, labels, solution, residual, direction, len_low, len_high, *scalars):
        features, width = points.shape
        height = features + 8
        vmem = pl.BlockSpec(memory_space=pltpu.VMEM)
        dma = pltpu.SemaphoreType.DMA
        operands = [points] + [
            value.reshape(1, -1)
            for value in (labels, residual, direction, len_low, len_high, *scalars)
        ]
        image, step_size, ratio = pl.pallas_call(
            functools.partial(kernel, row_count, col_count),
            out_shape=(jax.ShapeDtypeStruct((1, width), jnp.float32),) * 3,
            in_specs=[pl.BlockSpec(memory_space=pltpu.HBM)] * len(operands),
            out_specs=(vmem,) * 3,
            scratch_shapes=[pltpu.VMEM(value.shape, value.dtype) for value in operands[1:]]
            + [
                dma((len(operands),)),
                pltpu.VMEM((row_count, height, width), jnp.float32),
                pltpu.VMEM((col_count, height, width), jnp.float32),
                pltpu.VMEM((2, row_count, width, 4 * features), jnp.bfloat16),
                pltpu.VMEM((2, 4 * features, width), jnp.bfloat16),
                pltpu.VMEM((2, row_count, width, LANES), jnp.float32),
                pltpu.VMEM((2, row_count, width, LANES), jnp.float32),
                pltpu.VMEM((col_count, col_count, 1, width), jnp.float32),
                pltpu.VMEM((row_count, 4, LANES), jnp.float32),
                dma((row_count,)),
                dma((row_count,)),
                dma((col_count,)),
                dma((col_count,)),
                dma((col_count, col_count)),
                dma((col_count, col_count)),
                dma((row_count,)),
                dma((row_count,)),
            ],
            compiler_params=pltpu.CompilerParams(
                collective_id=0, has_side_effects=True
            ),
        )(*operands)
        image, step_size, ratio = (value.reshape(-1) for value in (image, step_size, ratio))
        residual_next = residual - step_size * image
        return solution + step_size * direction, residual_next, residual_next + ratio * direction

    spread = P(("row", "col"))
    return jax.shard_map(
        body,
        mesh=mesh,
        in_specs=(P(None, ("row", "col")), spread, spread, spread, spread) + (P(),) * 5,
        out_specs=(spread,) * 3,
        check_vma=False,
    )
```
